32 devices in a mesh: groups: 2 (over y), seq: 4 (over z), batch: 2 (over x), head: 2 (over core).
Axes of the slice: x: 2, y: 2, z: 4, core: 2. Of those that a mesh axis runs over, the one named last changes fastest.
Arguments:
- queries: bfloat16 [64, 64, 128], P(('groups', 'seq', 'batch'), 'head'), parts along dimension 0, may hold values from -16 to 16
- fresh_token_keys: bfloat16 [64, 8, 128], P(('groups', 'seq', 'batch'), 'head'), parts along dimension 0, may hold values from -12 to 12
- fresh_token_values: bfloat16 [64, 8, 128], P(('groups', 'seq', 'batch'), 'head'), parts along dimension 0, may hold values from -6 to 6
- shared_prefix_keys: bfloat16 [16384, 8, 128], P(('groups', 'seq'), 'head'), parts along dimension 0, may hold values from -6 to 6
- shared_prefix_values: bfloat16 [16384, 8, 128], P(('groups', 'seq'), 'head'), parts along dimension 0, may hold values from -6 to 6
- sequence_suffix_keys: bfloat16 [64, 192, 8, 128], P(('groups', 'seq', 'batch'), None, 'head'), parts along dimension 0, may hold values from -8 to 8
- sequence_suffix_values: bfloat16 [64, 192, 8, 128], P(('groups', 'seq', 'batch'), None, 'head'), parts along dimension 0, may hold values from -6 to 6
- suffix_lengths: int32 [64], P(('groups', 'seq', 'batch')), parts along dimension 0, may hold values from 0 to 192, as said below
Outputs:
- context: bfloat16 [64, 64, 128], P(('groups', 'seq', 'batch'), 'head'), parts along dimension 0
The draws below stay inside these ranges and needn't reach their ends.
There are 2 independent parts, one for each index of `groups`. The reference program is written for one: setup_inputs(seed, part) draws one part's arguments, and reference() takes and returns one part's arrays. A program takes and returns all parts, laid end to end along the dimension named above; each array names one. Nothing has to cross between parts.
Inputs may be any that keep to these rules, and one draw needn't show every extreme that they name: `suffix_lengths`: slots at and beyond a sequence's length hold no token. Some sequence has all 192 slots live in every draw.
All inputs are finite; a program needn't handle non-finite values.
Results may differ from the reference program's by a relative error of at most 0.002.
Values may be sent and summed in bfloat16 or wider, within the bound.
A program may use at most 64 MiB of HBM per device.

```python
import math
import jax
import jax.numpy as jnp
from jax import lax

QUERY_HEADS = 64
KEY_VALUE_HEADS = 8
HEAD_WIDTH = 128
PREFIX_PER_SHARD = 2048
SUFFIX_CAPACITY = 192
SEQUENCE_BATCH = 32
PREFIX_LENGTH = 8192
N_SEQ = 4


def draw_queries(key, part):
    start_offset = jnp.clip(jax.random.normal(jax.random.fold_in(key, 1), (SEQUENCE_BATCH, QUERY_HEADS, HEAD_WIDTH)) * 3.0, -16.0, 16.0)
    return start_offset.astype(jnp.bfloat16)


def draw_shared_prefix_keys(key, part):
    start_offset = jnp.clip(jax.random.normal(jax.random.fold_in(key, 3), (PREFIX_LENGTH, KEY_VALUE_HEADS, HEAD_WIDTH)), -6.0, 6.0)
    return start_offset.astype(jnp.bfloat16)


def draw_suffix_lengths(key, part):
    short_len = jax.random.randint(jax.random.fold_in(key, 21), (SEQUENCE_BATCH,), 0, SUFFIX_CAPACITY // 4 + 1)
    long_len = jax.random.randint(jax.random.fold_in(key, 22), (SEQUENCE_BATCH,), SUFFIX_CAPACITY // 2, SUFFIX_CAPACITY + 1)
    heavy = jax.random.randint(jax.random.fold_in(key, 23), (SEQUENCE_BATCH,), 0, 8) == 0
    lengths = jnp.where(heavy, long_len, short_len)
    chosen = jax.random.randint(jax.random.fold_in(key, 24), (), 0, SEQUENCE_BATCH)
    lengths = jnp.where(jnp.arange(SEQUENCE_BATCH, dtype=jnp.int32) == chosen, SUFFIX_CAPACITY, lengths)
    return lengths.astype(jnp.int32)


def block_scale(key, extent, cuts, smallest, top_value):
    def one(dim, shards_of):
        heights = jax.random.uniform(jax.random.fold_in(jax.random.fold_in(key, 6), dim), (shards_of,), jnp.float32, smallest / len(cuts), top_value / len(cuts))
        return jnp.repeat(jnp.exp(heights), extent[dim] // shards_of).reshape((-1,) + (1,) * (len(extent) - dim - 1))

    factor_of = one(*cuts[0])
    for cut in cuts[1:]:
        factor_of = factor_of * one(*cut)
    return factor_of


def centred(stream_key, shape, deviation, reach, pieces=(), kind=jnp.bfloat16):
    gain = block_scale(stream_key, shape, pieces, -0.22, 0.18) if pieces else 1.0
    entries = jax.random.normal(stream_key, shape, jnp.float32) * deviation * gain
    return jnp.minimum(jnp.maximum(entries, -reach), reach).astype(kind)


def setup_inputs(seed: int = 0, part: int = 0) -> dict:
    key_of = jax.random.split(jax.random.key(seed), 9)
    own_keys = jax.random.split(jax.random.fold_in(key_of[8], part), 9)
    return {
        "queries": draw_queries(jax.random.fold_in(jax.random.fold_in(key_of[8], part), 71), part),
        "fresh_token_keys": centred(own_keys[1], (SEQUENCE_BATCH, KEY_VALUE_HEADS, HEAD_WIDTH), 2.0, 12.0, ((0, 8), (1, 2))),
        "fresh_token_values": centred(own_keys[2], (SEQUENCE_BATCH, KEY_VALUE_HEADS, HEAD_WIDTH), 1.0, 6.0, ((0, 8), (1, 2))),
        "shared_prefix_keys": draw_shared_prefix_keys(jax.random.fold_in(jax.random.fold_in(key_of[8], part), 71), part),
        "shared_prefix_values": centred(own_keys[4], (PREFIX_LENGTH, KEY_VALUE_HEADS, HEAD_WIDTH), 1.0, 6.0, ((0, 4), (1, 2))),
        "sequence_suffix_keys": centred(own_keys[5], (SEQUENCE_BATCH, SUFFIX_CAPACITY, KEY_VALUE_HEADS, HEAD_WIDTH), 1.4, 8.0, ((0, 8), (2, 2))),
        "sequence_suffix_values": centred(own_keys[6], (SEQUENCE_BATCH, SUFFIX_CAPACITY, KEY_VALUE_HEADS, HEAD_WIDTH), 1.0, 6.0, ((0, 8), (2, 2))),
        "suffix_lengths": draw_suffix_lengths(jax.random.fold_in(jax.random.fold_in(key_of[8], part), 71), part),
    }


def prefix_state(query_single_precision, block_keys, block_values, inv_root):
    scores = jnp.einsum('bgqd,tgd->bgqt', query_single_precision, block_keys.astype(jnp.float32)) * inv_root
    maxima = lax.optimization_barrier(jnp.max(scores, axis=-1))
    weights = jnp.exp(scores - maxima[..., None]).astype(jnp.bfloat16)
    totals = lax.optimization_barrier(jnp.sum(weights.astype(jnp.float32), axis=-1))
    outputs = jnp.einsum('bgqt,tgd->bgqd', weights.astype(jnp.float32), block_values.astype(jnp.float32))
    return (maxima, totals, outputs)

def reference(queries, fresh_token_keys, fresh_token_values, shared_prefix_keys, shared_prefix_values, sequence_suffix_keys, sequence_suffix_values, suffix_lengths):
    query_group = QUERY_HEADS // KEY_VALUE_HEADS
    inv_root = 1.0 / math.sqrt(HEAD_WIDTH)
    query_single_precision = queries.astype(jnp.float32).reshape(SEQUENCE_BATCH, KEY_VALUE_HEADS, query_group, HEAD_WIDTH)
    own_scores = jnp.einsum('bgqd,bgd->bgq', query_single_precision, fresh_token_keys.astype(jnp.float32)) * inv_root
    recent = jnp.einsum('bgqd,bsgd->bgqs', query_single_precision, sequence_suffix_keys.astype(jnp.float32)) * inv_root
    live = (jnp.arange(SUFFIX_CAPACITY, dtype=jnp.int32)[None, :] < suffix_lengths.astype(jnp.int32)[:, None])[:, None, None, :]
    local_max = jnp.maximum(own_scores, lax.optimization_barrier(jnp.max(jnp.where(live, recent, own_scores[..., None]), axis=-1)))
    recent_weights = jnp.where(live, jnp.exp(jnp.where(live, recent - local_max[..., None], 0.0)), 0.0).astype(jnp.bfloat16)
    own_weights = jnp.exp(own_scores - local_max).astype(jnp.bfloat16)
    local_total = lax.optimization_barrier(jnp.sum(recent_weights.astype(jnp.float32), axis=-1)) + own_weights.astype(jnp.float32)
    local_out = jnp.einsum('bgqs,bsgd->bgqd', recent_weights.astype(jnp.float32), sequence_suffix_values.astype(jnp.float32))
    local_out = local_out + own_weights.astype(jnp.float32)[..., None] * fresh_token_values.astype(jnp.float32)[:, :, None, :]
    keys_divided = shared_prefix_keys.reshape(N_SEQ, PREFIX_PER_SHARD, KEY_VALUE_HEADS, HEAD_WIDTH)
    values_divided = shared_prefix_values.reshape(N_SEQ, PREFIX_PER_SHARD, KEY_VALUE_HEADS, HEAD_WIDTH)

    def absorb(carry, block):
        running_max, running_total, running_out = carry
        maxima, totals, outputs = prefix_state(query_single_precision, block[0], block[1], inv_root)
        highest = jnp.maximum(running_max, maxima)
        old_scale = jnp.exp(running_max - highest)
        new_scale = jnp.exp(maxima - highest)
        merged_total = running_total * old_scale + totals * new_scale
        merged_out = running_out * old_scale[..., None] + outputs * new_scale[..., None]
        return ((highest, merged_total, merged_out), None)
    (final_max, total, numerator), unused = lax.scan(absorb, (local_max, local_total, local_out), (keys_divided, values_divided))
    return (numerator / total[..., None]).astype(jnp.bfloat16).reshape(SEQUENCE_BATCH, QUERY_HEADS, HEAD_WIDTH)
```

```python
import functools
import math

import jax
import jax.numpy as jnp
from jax import lax
from jax.experimental import pallas as pl
from jax.experimental.pallas import tpu as pltpu
from jax.sharding import PartitionSpec as P

MESH = pl.DeviceIdType.MESH
BF16 = jnp.bfloat16
F32 = jnp.float32
CHUNKS = 4
LOOP_ROWS = 512


def kernel(
    n,
    kv,
    lengths_ref,
    q_ref,
    fk_ref,
    fv_ref,
    pk_hbm,
    pv_hbm,
    sk_hbm,
    sv_hbm,
    o_ref,
    kraw,
    vraw,
    wide,
    kh,
    vh,
    sk,
    sv,
    qown,
    qall,
    obuf,
    rbuf,
    lo_s,
    lm_s,
    ll_s,
    pre_sem,
    suf_sem,
    qsend,
    qrecv,
    osend,
    orecv,
):
    own, heads, width = q_ref.shape
    group = heads // kv
    rows = own * group
    total_rows = pk_hbm.shape[0]
    positions = total_rows // kv
    chunk = total_rows // CHUNKS
    slots = sk_hbm.shape[1] // kv
    scale = math.log2(math.e) / math.sqrt(width)
    me = lax.axis_index("seq")
    peers = [lax.rem(me + d, n) for d in range(1, n)]

    barrier = pltpu.get_barrier_semaphore()
    for peer in peers:
        pl.semaphore_signal(barrier, inc=1, device_id={"seq": peer}, device_id_type=MESH)

    def prefix_copy(which, c):
        src, dst = ((pk_hbm, kraw), (pv_hbm, vraw))[which]
        span = pl.ds(c * chunk, chunk)
        return pltpu.make_async_copy(src.at[span], dst.at[span], pre_sem.at[which, c])

    suffix_copies = [
        pltpu.make_async_copy(sk_hbm, sk, suf_sem.at[0]),
        pltpu.make_async_copy(sv_hbm, sv, suf_sem.at[1]),
    ]
    for c in range(CHUNKS):
        prefix_copy(0, c).start()
    for copy in suffix_copies:
        copy.start()
    for c in range(CHUNKS):
        prefix_copy(1, c).start()

    q32 = [q_ref[b].astype(F32) for b in range(own)]
    for g in range(kv):
        part = jnp.concatenate([q32[b][g * group : (g + 1) * group] for b in range(own)], axis=0)
        part = part.astype(BF16)
        qown[g] = part
        qall[g, me] = part

    pl.semaphore_wait(barrier, n - 1)

    def query_copy(g, peer):
        return pltpu.make_async_remote_copy(
            src_ref=qown.at[g],
            dst_ref=qall.at[g, me],
            send_sem=qsend.at[g, peer],
            recv_sem=qrecv.at[g, me],
            device_id={"seq": peer},
            device_id_type=MESH,
        )

    def query_arrival(g, peer):
        return pltpu.make_async_remote_copy(
            src_ref=qown.at[g],
            dst_ref=qall.at[g, peer],
            send_sem=qsend.at[g, peer],
            recv_sem=qrecv.at[g, peer],
            device_id={"seq": peer},
            device_id_type=MESH,
        )

    for g in range(kv):
        for peer in peers:
            query_copy(g, peer).start()

    def split_heads(raw, out, c):
        per = LOOP_ROWS // kv

        @pl.loop(0, chunk // LOOP_ROWS)
        def _(i):
            base = pl.multiple_of(c * chunk + i * LOOP_ROWS, LOOP_ROWS)
            wide[...] = raw[pl.ds(base, LOOP_ROWS), :].astype(F32)
            first = pl.multiple_of((c * chunk) // kv + i * per, per)
            for g in range(kv):
                out[g, pl.ds(first, per), :] = wide[pl.ds(g, per, stride=kv), :].astype(BF16)

    for c in range(CHUNKS):
        prefix_copy(0, c).wait()
        split_heads(kraw, kh, c)

    for copy in suffix_copies:
        copy.wait()
    columns = slots * kv
    col = lax.broadcasted_iota(jnp.int32, (heads, columns), 1)
    row = lax.broadcasted_iota(jnp.int32, (heads, columns), 0)
    same_head = lax.rem(col, kv) == row // group
    slot = col // kv
    for b in range(own):
        live = jnp.logical_and(same_head, slot < lengths_ref[b])
        fk = fk_ref[b].astype(F32)
        fv = fv_ref[b].astype(F32)
        fk_rows = jnp.concatenate(
            [jnp.broadcast_to(fk[g : g + 1], (group, width)) for g in range(kv)], axis=0
        )
        fv_rows = jnp.concatenate(
            [jnp.broadcast_to(fv[g : g + 1], (group, width)) for g in range(kv)], axis=0
        )
        own_score = jnp.sum(q32[b] * fk_rows, axis=1, keepdims=True) * scale
        s = (
            lax.dot_general(
                q_ref[b], sk[b], (((1,), (1,)), ((), ())), preferred_element_type=F32
            )
            * scale
        )
        s = jnp.where(live, s, own_score)
        top = jnp.maximum(jnp.max(s, axis=1, keepdims=True), own_score)
        p = jnp.where(live, jnp.exp2(s - top), 0.0).astype(BF16)
        w = jnp.exp2(own_score - top).astype(BF16).astype(F32)
        total = jnp.sum(p.astype(F32), axis=1, keepdims=True) + w
        out = jnp.dot(p, sv[b], preferred_element_type=F32) + w * fv_rows
        top = jnp.broadcast_to(top, (heads, width))
        total = jnp.broadcast_to(total, (heads, width))
        for g in range(kv):
            dst = pl.ds(b * group, group)
            src = slice(g * group, (g + 1) * group)
            lo_s[g, dst, :] = out[src]
            lm_s[g, dst, :] = top[src]
            ll_s[g, dst, :] = total[src]

    for c in range(CHUNKS):
        prefix_copy(1, c).wait()
        split_heads(vraw, vh, c)

    lane = lax.broadcasted_iota(jnp.int32, (rows, width), 1)
    line = lax.broadcasted_iota(jnp.int32, (rows, width), 0)
    is_max = lane == line
    is_total = lane == line + rows

    def out_copy(g, peer):
        return pltpu.make_async_remote_copy(
            src_ref=obuf.at[g, peer],
            dst_ref=rbuf.at[g, me],
            send_sem=osend.at[g, peer],
            recv_sem=orecv.at[g, me],
            device_id={"seq": peer},
            device_id_type=MESH,
        )

    def out_arrival(g, peer):
        return pltpu.make_async_remote_copy(
            src_ref=obuf.at[g, peer],
            dst_ref=rbuf.at[g, peer],
            send_sem=osend.at[g, peer],
            recv_sem=orecv.at[g, peer],
            device_id={"seq": peer},
            device_id_type=MESH,
        )

    def scores(g):
        for peer in peers:
            query_arrival(g, peer).wait_recv()
        return lax.dot_general(
            qall[g].reshape(n * rows, width),
            kh[g],
            (((1,), (1,)), ((), ())),
            preferred_element_type=F32,
        )

    for g in range(kv):
        s = scores(g) * scale
        top = jnp.max(s, axis=1, keepdims=True)
        p = jnp.exp2(s - top).astype(BF16)
        total = jnp.sum(p.astype(F32), axis=1, keepdims=True)
        out = jnp.dot(p, vh[g], preferred_element_type=F32)
        for j in range(n):
            block = slice(j * rows, (j + 1) * rows)
            obuf[g, j, 0:rows, :] = out[block]
            stats = jnp.where(is_max, top[block], jnp.where(is_total, total[block], 0.0))
            obuf[g, j, rows : rows + 1, :] = jnp.sum(stats, axis=0, keepdims=True)
        for peer in peers:
            out_copy(g, peer).start()

    def columns_of(stat):
        wide_stat = jnp.broadcast_to(stat, (rows, width))
        m = jnp.sum(jnp.where(is_max, wide_stat, 0.0), axis=1, keepdims=True)
        t = jnp.sum(jnp.where(is_total, wide_stat, 0.0), axis=1, keepdims=True)
        return m, t

    for g in range(kv):
        for peer in peers:
            out_arrival(g, peer).wait_recv()
        parts = [(obuf, me)] + [(rbuf, peer) for peer in peers]
        stats = [columns_of(buf[g, j, rows : rows + 1, :]) for buf, j in parts]
        lm = lm_s[g]
        highest = lm
        for m, _ in stats:
            highest = jnp.maximum(highest, m)
        local_scale = jnp.exp2(lm - highest)
        total = ll_s[g] * local_scale
        numerator = lo_s[g] * local_scale
        for (buf, j), (m, t) in zip(parts, stats):
            factor = jnp.exp2(m - highest)
            total = total + t * factor
            numerator = numerator + buf[g, j, 0:rows, :] * factor
        context = (numerator / total).astype(BF16)
        for b in range(own):
            o_ref[b, g * group : (g + 1) * group, :] = context[b * group : (b + 1) * group]

    for g in range(kv):
        for peer in peers:
            query_copy(g, peer).wait_send()
            out_copy(g, peer).wait_send()


def body(
    n,
    queries,
    fresh_token_keys,
    fresh_token_values,
    shared_prefix_keys,
    shared_prefix_values,
    sequence_suffix_keys,
    sequence_suffix_values,
    suffix_lengths,
):
    own, heads, width = queries.shape
    positions, kv, _ = shared_prefix_keys.shape
    slots = sequence_suffix_keys.shape[1]
    rows = own * (heads // kv)
    total_rows = positions * kv
    any_spec = pl.BlockSpec(memory_space=pl.ANY)
    vmem_spec = pl.BlockSpec(memory_space=pltpu.VMEM)
    return pl.pallas_call(
        functools.partial(kernel, n, kv),
        out_shape=jax.ShapeDtypeStruct(queries.shape, BF16),
        in_specs=[pl.BlockSpec(memory_space=pltpu.SMEM)] + [vmem_spec] * 3 + [any_spec] * 4,
        out_specs=vmem_spec,
        scratch_shapes=[
            pltpu.VMEM((total_rows, width), BF16),
            pltpu.VMEM((total_rows, width), BF16),
            pltpu.VMEM((LOOP_ROWS, width), F32),
            pltpu.VMEM((kv, positions, width), BF16),
            pltpu.VMEM((kv, positions, width), BF16),
            pltpu.VMEM((own, slots * kv, width), BF16),
            pltpu.VMEM((own, slots * kv, width), BF16),
            pltpu.VMEM((kv, rows, width), BF16),
            pltpu.VMEM((kv, n, rows, width), BF16),
            pltpu.VMEM((kv, n, rows + 1, width), F32),
            pltpu.VMEM((kv, n, rows + 1, width), F32),
            pltpu.VMEM((kv, rows, width), F32),
            pltpu.VMEM((kv, rows, width), F32),
            pltpu.VMEM((kv, rows, width), F32),
            pltpu.SemaphoreType.DMA((2, CHUNKS)),
            pltpu.SemaphoreType.DMA((2,)),
            pltpu.SemaphoreType.DMA((kv, n)),
            pltpu.SemaphoreType.DMA((kv, n)),
            pltpu.SemaphoreType.DMA((kv, n)),
            pltpu.SemaphoreType.DMA((kv, n)),
        ],
        compiler_params=pltpu.CompilerParams(
            collective_id=0, has_side_effects=True, vmem_limit_bytes=60 * 1024 * 1024
        ),
        name="decode_attention",
    )(
        suffix_lengths,
        queries,
        fresh_token_keys,
        fresh_token_values,
        shared_prefix_keys.reshape(total_rows, width),
        shared_prefix_values.reshape(total_rows, width),
        sequence_suffix_keys.reshape(own, slots * kv, width),
        sequence_suffix_values.reshape(own, slots * kv, width),
    )


def solution(mesh):
    in_specs = (
        P(("groups", "seq", "batch"), "head", None),
        P(("groups", "seq", "batch"), "head", None),
        P(("groups", "seq", "batch"), "head", None),
        P(("groups", "seq"), "head", None),
        P(("groups", "seq"), "head", None),
        P(("groups", "seq", "batch"), None, "head", None),
        P(("groups", "seq", "batch"), None, "head", None),
        P(("groups", "seq", "batch")),
    )
    out_specs = P(("groups", "seq", "batch"), "head", None)
    return jax.shard_map(
        functools.partial(body, mesh.shape["seq"]),
        mesh=mesh,
        in_specs=in_specs,
        out_specs=out_specs,
        check_vma=False,
    )
```

```python
import functools
import math

import jax
import jax.numpy as jnp
from jax import lax
from jax.experimental import pallas as pl
from jax.experimental.pallas import tpu as pltpu
from jax.sharding import PartitionSpec as P

MESH = pl.DeviceIdType.MESH
BF16 = jnp.bfloat16
F32 = jnp.float32
CHUNKS = 4
LOOP_ROWS = 512
CODE_MAX = 32767.0
QUERY_HEADS = 2
VMEM_BYTES = 60 * 1024 * 1024


def kernel(
    n,
    kv,
    lengths_hbm,
    q_hbm,
    fk_hbm,
    fv_hbm,
    pk_hbm,
    pv_hbm,
    sk_hbm,
    sv_hbm,
    o_ref,
    lengths_ref,
    q_ref,
    fk_ref,
    fv_ref,
    kraw,
    vraw,
    wide,
    kh,
    vh,
    sk,
    sv,
    qown,
    qall,
    obuf,
    rbuf,
    ostat,
    rstat,
    lo_s,
    lm_s,
    ll_s,
    small_sem,
    pre_sem,
    suf_sem,
    qsend,
    qrecv,
    osend,
    orecv,
    ssend,
    srecv,
):
    own, heads, width = q_hbm.shape
    group = heads // kv
    rows = own * group
    half = rows // 2
    total_rows = pk_hbm.shape[0]
    positions = total_rows // kv
    chunk = total_rows // CHUNKS
    slots = sk_hbm.shape[1] // kv
    scale = math.log2(math.e) / math.sqrt(width)
    me = lax.axis_index("seq")
    peers = [lax.rem(me + d, n) for d in range(1, n)]

    barrier = pltpu.get_barrier_semaphore()
    for peer in peers:
        pl.semaphore_signal(barrier, inc=1, device_id={"seq": peer}, device_id_type=MESH)

    small_copies = [
        pltpu.make_async_copy(src, dst, small_sem.at[i])
        for i, (src, dst) in enumerate(
            ((q_hbm, q_ref), (fk_hbm, fk_ref), (fv_hbm, fv_ref), (lengths_hbm, lengths_ref))
        )
    ]
    for copy in small_copies:
        copy.start()

    def prefix_copy(which, c):
        src, dst = ((pk_hbm, kraw), (pv_hbm, vraw))[which]
        span = pl.ds(c * chunk, chunk)
        return pltpu.make_async_copy(src.at[span], dst.at[span], pre_sem.at[which, c])

    suffix_copies = [
        pltpu.make_async_copy(sk_hbm, sk, suf_sem.at[0]),
        pltpu.make_async_copy(sv_hbm, sv, suf_sem.at[1]),
    ]
    for c in range(CHUNKS):
        prefix_copy(0, c).start()
    for copy in suffix_copies:
        copy.start()
    for c in range(CHUNKS):
        prefix_copy(1, c).start()

    small_copies[0].wait()
    q32 = [q_ref[b].astype(F32) for b in range(own)]
    for g in range(kv):
        part = jnp.concatenate([q32[b][g * group : (g + 1) * group] for b in range(own)], axis=0)
        part = part.astype(BF16)
        qown[g] = part

    pl.semaphore_wait(barrier, n - 1)

    def query_copy(h, d, slot):
        span = pl.ds(h * QUERY_HEADS, QUERY_HEADS)
        return pltpu.make_async_remote_copy(
            src_ref=qown.at[span],
            dst_ref=qall.at[slot, span],
            send_sem=qsend.at[h, d - 1],
            recv_sem=qrecv.at[h, slot],
            device_id={"seq": peers[d - 1]},
            device_id_type=MESH,
        )

    query_parts = kv // QUERY_HEADS
    for h in range(query_parts):
        for d in range(1, n):
            query_copy(h, d, n - d - 1).start()

    def split_heads(raw, out, c):
        per = LOOP_ROWS // kv

        @pl.loop(0, chunk // LOOP_ROWS)
        def _(i):
            base = pl.multiple_of(c * chunk + i * LOOP_ROWS, LOOP_ROWS)
            wide[...] = raw[pl.ds(base, LOOP_ROWS), :].astype(F32)
            first = pl.multiple_of((c * chunk) // kv + i * per, per)
            for g in range(kv):
                out[g, pl.ds(first, per), :] = wide[pl.ds(g, per, stride=kv), :].astype(BF16)

    for c in range(CHUNKS):
        prefix_copy(0, c).wait()
        split_heads(kraw, kh, c)

    for copy in suffix_copies + small_copies[1:]:
        copy.wait()
    columns = slots * kv
    col = lax.broadcasted_iota(jnp.int32, (heads, columns), 1)
    row = lax.broadcasted_iota(jnp.int32, (heads, columns), 0)
    same_head = lax.rem(col, kv) == row // group
    slot = col // kv
    for b in range(own):
        live = jnp.logical_and(same_head, slot < lengths_ref[b])
        fk = fk_ref[b].astype(F32)
        fv = fv_ref[b].astype(F32)
        fk_rows = jnp.concatenate(
            [jnp.broadcast_to(fk[g : g + 1], (group, width)) for g in range(kv)], axis=0
        )
        fv_rows = jnp.concatenate(
            [jnp.broadcast_to(fv[g : g + 1], (group, width)) for g in range(kv)], axis=0
        )
        own_score = jnp.sum(q32[b] * fk_rows, axis=1, keepdims=True) * scale
        s = (
            lax.dot_general(
                q_ref[b], sk[b], (((1,), (1,)), ((), ())), preferred_element_type=F32
            )
            * scale
        )
        s = jnp.where(live, s, own_score)
        top = jnp.maximum(jnp.max(s, axis=1, keepdims=True), own_score)
        p = jnp.where(live, jnp.exp2(s - top), 0.0).astype(BF16)
        w = jnp.exp2(own_score - top).astype(BF16).astype(F32)
        total = jnp.sum(p.astype(F32), axis=1, keepdims=True) + w
        out = jnp.dot(p, sv[b], preferred_element_type=F32) + w * fv_rows
        top = jnp.broadcast_to(top, (heads, width))
        total = jnp.broadcast_to(total, (heads, width))
        for g in range(kv):
            dst = pl.ds(b * group, group)
            src = slice(g * group, (g + 1) * group)
            lo_s[g, dst, :] = out[src]
            lm_s[g, dst, :] = top[src]
            ll_s[g, dst, :] = total[src]

    for c in range(CHUNKS):
        prefix_copy(1, c).wait()
        split_heads(vraw, vh, c)

    lane = lax.broadcasted_iota(jnp.int32, (rows, width), 1)
    line = lax.broadcasted_iota(jnp.int32, (rows, width), 0)
    is_max = lane == line
    is_total = lane == line + rows
    is_size = lane == line + 2 * rows

    def returns(g, d, slot):
        return [
            pltpu.make_async_remote_copy(
                src_ref=src.at[g, d - 1],
                dst_ref=dst.at[g, slot],
                send_sem=send.at[g, d - 1],
                recv_sem=recv.at[g, slot],
                device_id={"seq": peers[d - 1]},
                device_id_type=MESH,
            )
            for src, dst, send, recv in (
                (ostat, rstat, ssend, srecv),
                (obuf, rbuf, osend, orecv),
            )
        ]

    def attend(s, g):
        s = s * scale
        top = jnp.max(s, axis=1, keepdims=True)
        p = jnp.exp2(s - top).astype(BF16)
        total = jnp.sum(p.astype(F32), axis=1, keepdims=True)
        return top, total, jnp.dot(p, vh[g], preferred_element_type=F32)

    def scores(g, query_rows):
        return lax.dot_general(
            query_rows, kh[g], (((1,), (1,)), ((), ())), preferred_element_type=F32
        )

    def remote_scores(g):
        if g % QUERY_HEADS == 0:
            for d in range(1, n):
                query_copy(g // QUERY_HEADS, d, d - 1).wait_recv()
        return scores(g, jnp.concatenate([qall[d - 1, g] for d in range(1, n)], axis=0))

    own_next = scores(0, qown[0])
    for g in range(kv):
        s = own_next
        if g + 1 < kv:
            own_next = scores(g + 1, qown[g + 1])
        top, total, out = attend(s, g)
        lm = lm_s[g]
        highest = jnp.maximum(lm, top)
        local_scale = jnp.exp2(lm - highest)
        block_scale = jnp.exp2(top - highest)
        lm_s[g] = highest
        ll_s[g] = ll_s[g] * local_scale + total * block_scale
        lo_s[g] = lo_s[g] * local_scale + out * block_scale

    following = remote_scores(0)
    for g in range(kv):
        s = following
        if g + 1 < kv:
            following = remote_scores(g + 1)
        top, total, out = attend(s, g)
        size = jnp.maximum(jnp.max(jnp.abs(out), axis=1, keepdims=True), 1e-30)
        coded = jnp.floor(out * (CODE_MAX / size) + 0.5).astype(jnp.int32)
        for d in range(1, n):
            block = slice((d - 1) * rows, d * rows)
            stats = jnp.where(is_max, top[block], jnp.where(is_total, total[block], 0.0))
            stats = jnp.where(is_size, size[block], stats)
            ostat[g, d - 1] = jnp.sum(stats, axis=0, keepdims=True)
            high = coded[(d - 1) * rows : (d - 1) * rows + half]
            low = coded[(d - 1) * rows + half : d * rows]
            obuf[g, d - 1] = (high << 16) | (low & 0xFFFF)
        for d in range(1, n):
            for copy in returns(g, d, n - d - 1):
                copy.start()

    def columns_of(stat):
        wide_stat = jnp.broadcast_to(stat, (rows, width))
        return [
            jnp.sum(jnp.where(mask, wide_stat, 0.0), axis=1, keepdims=True)
            for mask in (is_max, is_total, is_size)
        ]

    for g in range(kv):
        for d in range(1, n):
            for copy in returns(g, d, d - 1):
                copy.wait_recv()
        stats = [columns_of(rstat[g, d - 1]) for d in range(1, n)]
        lm = lm_s[g]
        highest = lm
        for m, _, _ in stats:
            highest = jnp.maximum(highest, m)
        local_scale = jnp.exp2(lm - highest)
        total = ll_s[g] * local_scale
        numerator = lo_s[g] * local_scale
        for d, (m, t, a) in enumerate(stats, 1):
            factor = jnp.exp2(m - highest)
            total = total + t * factor
            words = rbuf[g, d - 1]
            codes = jnp.concatenate([words >> 16, (words << 16) >> 16], axis=0)
            numerator = numerator + codes.astype(F32) * (a * (factor * (1.0 / CODE_MAX)))
        context = (numerator / total).astype(BF16)
        for b in range(own):
            o_ref[b, g * group : (g + 1) * group, :] = context[b * group : (b + 1) * group]

    for d in range(1, n):
        for h in range(query_parts):
            query_copy(h, d, n - d - 1).wait_send()
        for g in range(kv):
            for copy in returns(g, d, n - d - 1):
                copy.wait_send()


def body(
    n,
    queries,
    fresh_token_keys,
    fresh_token_values,
    shared_prefix_keys,
    shared_prefix_values,
    sequence_suffix_keys,
    sequence_suffix_values,
    suffix_lengths,
):
    own, heads, width = queries.shape
    positions, kv, _ = shared_prefix_keys.shape
    slots = sequence_suffix_keys.shape[1]
    rows = own * (heads // kv)
    total_rows = positions * kv
    hbm_spec = pl.BlockSpec(memory_space=pltpu.HBM)
    vmem_spec = pl.BlockSpec(memory_space=pltpu.VMEM)
    return pl.pallas_call(
        functools.partial(kernel, n, kv),
        out_shape=jax.ShapeDtypeStruct(queries.shape, BF16),
        in_specs=[hbm_spec] * 8,
        out_specs=vmem_spec,
        scratch_shapes=[
            pltpu.SMEM(suffix_lengths.shape, jnp.int32),
            pltpu.VMEM(queries.shape, BF16),
            pltpu.VMEM(fresh_token_keys.shape, BF16),
            pltpu.VMEM(fresh_token_values.shape, BF16),
            pltpu.VMEM((total_rows, width), BF16),
            pltpu.VMEM((total_rows, width), BF16),
            pltpu.VMEM((LOOP_ROWS, width), F32),
            pltpu.VMEM((kv, positions, width), BF16),
            pltpu.VMEM((kv, positions, width), BF16),
            pltpu.VMEM((own, slots * kv, width), BF16),
            pltpu.VMEM((own, slots * kv, width), BF16),
            pltpu.VMEM((kv, rows, width), BF16),
            pltpu.VMEM((n - 1, kv, rows, width), BF16),
            pltpu.VMEM((kv, n - 1, rows // 2, width), jnp.int32),
            pltpu.VMEM((kv, n - 1, rows // 2, width), jnp.int32),
            pltpu.VMEM((kv, n - 1, 1, width), F32),
            pltpu.VMEM((kv, n - 1, 1, width), F32),
            pltpu.VMEM((kv, rows, width), F32),
            pltpu.VMEM((kv, rows, width), F32),
            pltpu.VMEM((kv, rows, width), F32),
            pltpu.SemaphoreType.DMA((4,)),
            pltpu.SemaphoreType.DMA((2, CHUNKS)),
            pltpu.SemaphoreType.DMA((2,)),
            pltpu.SemaphoreType.DMA((kv, n - 1)),
            pltpu.SemaphoreType.DMA((kv, n - 1)),
            pltpu.SemaphoreType.DMA((kv, n - 1)),
            pltpu.SemaphoreType.DMA((kv, n - 1)),
            pltpu.SemaphoreType.DMA((kv, n - 1)),
            pltpu.SemaphoreType.DMA((kv, n - 1)),
        ],
        compiler_params=pltpu.CompilerParams(
            collective_id=0, has_side_effects=True, vmem_limit_bytes=VMEM_BYTES
        ),
        name="decode_attention",
    )(
        suffix_lengths,
        queries,
        fresh_token_keys,
        fresh_token_values,
        shared_prefix_keys.reshape(total_rows, width),
        shared_prefix_values.reshape(total_rows, width),
        sequence_suffix_keys.reshape(own, slots * kv, width),
        sequence_suffix_values.reshape(own, slots * kv, width),
    )


def solution(mesh):
    in_specs = (
        P(("groups", "seq", "batch"), "head", None),
        P(("groups", "seq", "batch"), "head", None),
        P(("groups", "seq", "batch"), "head", None),
        P(("groups", "seq"), "head", None),
        P(("groups", "seq"), "head", None),
        P(("groups", "seq", "batch"), None, "head", None),
        P(("groups", "seq", "batch"), None, "head", None),
        P(("groups", "seq", "batch")),
    )
    out_specs = P(("groups", "seq", "batch"), "head", None)
    return jax.shard_map(
        functools.partial(body, mesh.shape["seq"]),
        mesh=mesh,
        in_specs=in_specs,
        out_specs=out_specs,
        check_vma=False,
    )
```
